32 devices in a mesh: row: 4 (over x, core), col: 8 (over z, y).
Axes of the slice: x: 2, y: 2, z: 4, core: 2. Of those that a mesh axis runs over, the one named last changes fastest.
Arguments:
- source_terms: float32 [256, 512, 256], P('row', 'col'), may hold values from -6 to 6
- initial_values: float32 [256, 512, 256], P('row', 'col'), may hold values from -6 to 6
- absorption: float32 [256, 512, 256], P('row', 'col'), may hold values from 0.1 to 0.9
Outputs:
- improved: float32 [256, 512, 256], P('row', 'col')
- remaining: float32 [256, 512, 256], P('row', 'col')
The draws below stay inside these ranges and needn't reach their ends.
All inputs are finite; a program needn't handle non-finite values.
Results may differ from the reference program's by a relative error of at most 0.000043.
Values sent between devices are 32-bit elements; how exact they have to be, the bound alone decides.
A program may use at most 128 MiB of HBM per device.

```python
import jax
import jax.numpy as jnp
from jax import lax

LAYERS = 256
RATIO = 4
BEFORE = 3
AFTER = 3
INNER = 9
GRID_Y = 256
GRID_X = 512


def shard_levels(key, dims, split, smallest, top_value):
    def one(axis_at, shards_of):
        steps = jax.random.uniform(jax.random.fold_in(jax.random.fold_in(key, 6), axis_at), (shards_of,), jnp.float32, smallest / len(split), top_value / len(split))
        return jnp.repeat(jnp.exp(steps), dims[axis_at] // shards_of).reshape((-1,) + (1,) * (len(dims) - axis_at - 1))

    factor_of = one(*split[0])
    for cut in split[1:]:
        factor_of = factor_of * one(*cut)
    return factor_of


def normal_values(own_key, dims, spread, limit, split=(), held_as=jnp.bfloat16):
    values = jax.random.normal(own_key, dims, jnp.float32) * spread
    if len(split) > 0:
        values = shard_levels(own_key, dims, split, -0.22, 0.18) * values
    return jnp.clip(values, min=-limit, max=limit).astype(held_as)


def setup_inputs(seed: int = 0) -> dict:
    arg_keys = jax.random.split(jax.random.key(seed), 4)
    return {
        "source_terms": normal_values(arg_keys[0], (GRID_Y, GRID_X, LAYERS), 1.0, 6.0, ((0, 4), (1, 8)), jnp.float32),
        "initial_values": normal_values(arg_keys[1], (GRID_Y, GRID_X, LAYERS), 1.0, 6.0, ((0, 4), (1, 8)), jnp.float32),
        "absorption": jnp.clip(0.1 + 0.79999997 * jax.random.uniform(arg_keys[2], (GRID_Y, GRID_X, LAYERS), jnp.float32) ** shard_levels(arg_keys[2], (GRID_Y, GRID_X, LAYERS), ((0, 4), (1, 8)), -0.2, 0.2), 0.1, 0.9),
    }


def cross_sum(padded):
    inner_y, inner_x = padded.shape[0] - 2, padded.shape[1] - 2
    middle_rows = lax.slice_in_dim(padded, 1, 1 + inner_y, axis=0)
    middle_columns = lax.slice_in_dim(padded, 1, 1 + inner_x, axis=1)
    return (lax.slice_in_dim(middle_columns, 0, inner_y, axis=0) + lax.slice_in_dim(middle_columns, 2, 2 + inner_y, axis=0)
            + lax.slice_in_dim(middle_rows, 0, inner_x, axis=1) + lax.slice_in_dim(middle_rows, 2, 2 + inner_x, axis=1))


def smooth_step(padded, values, load, mass_here):
    return values + 0.8 * (load + cross_sum(padded) - (4.0 + mass_here) * values) / (4.0 + mass_here)


def block_means(values):
    cut = values.reshape(values.shape[0] // RATIO, RATIO, values.shape[1] // RATIO, RATIO, values.shape[2])
    return jnp.mean(cut, axis=(1, 3))


def spread_blocks(values):
    return jnp.repeat(jnp.repeat(values, RATIO, axis=0), RATIO, axis=1)


def reference(source_terms, initial_values, absorption):
    values = initial_values
    for sweep in range(BEFORE):
        values = smooth_step(jnp.pad(values, ((1, 1), (1, 1), (0, 0)), mode="wrap"), values, source_terms, absorption)
    defect = source_terms + cross_sum(jnp.pad(values, ((1, 1), (1, 1), (0, 0)), mode="wrap")) - (4.0 + absorption) * values
    coarse_load, coarse_mass = block_means(defect) * RATIO, block_means(absorption) * RATIO
    coarse_values = jnp.zeros_like(coarse_load)
    for sweep in range(INNER):
        coarse_values = smooth_step(jnp.pad(coarse_values, ((1, 1), (1, 1), (0, 0)), mode="wrap"), coarse_values, coarse_load, coarse_mass)
    values = values + spread_blocks(coarse_values)
    for sweep in range(AFTER):
        values = smooth_step(jnp.pad(values, ((1, 1), (1, 1), (0, 0)), mode="wrap"), values, source_terms, absorption)
    improved = values
    remaining = source_terms + cross_sum(jnp.pad(improved, ((1, 1), (1, 1), (0, 0)), mode="wrap")) - (4.0 + absorption) * improved
    return improved, remaining
```

```python
import functools

import jax
import jax.numpy as jnp
from jax import lax
from jax.experimental import pallas as pl
from jax.experimental.pallas import tpu as pltpu
from jax.sharding import PartitionSpec as P

RATIO = 4
INNER = 9
DEEP = 2
WIDE = 4
TILE = 8
LANES = 128
MESH = pl.DeviceIdType.MESH
SIDES = ((-1, 0), (1, 0), (0, -1), (0, 1))
CORNERS = ((-1, -1), (-1, 1), (1, -1), (1, 1))
AROUND = SIDES + CORNERS


def span(step, length, depth):
    if step == 0:
        return 0, 0, length
    if step < 0:
        return 0, length, depth
    return length - depth, -depth, depth


def kernel(rows, cols, ny, nx, nl, f_hbm, u_hbm, m_hbm, out_hbm, rem_hbm, a, b, c, f, m, w, cl, cm, cw, v0, v1, v5,
           send, recv, local):
    me_r, me_c = lax.axis_index("row"), lax.axis_index("col")
    cy, cx = ny // RATIO, nx // RATIO
    wide_x, wide_cx = nx + TILE, cx + TILE

    def device(dy, dx):
        return (lax.rem(me_r + (dy + rows), rows), lax.rem(me_c + (dx + cols), cols))

    barrier = pltpu.get_barrier_semaphore()
    for dy, dx in AROUND:
        pl.semaphore_signal(barrier, inc=1, device_id=device(dy, dx), device_id_type=MESH)

    used = [0]

    def send_to(dy, dx, src, dst, depth, length_y, length_x, off_src, off_dst):
        width = length_x + TILE
        y_from, y_to, y_n = span(dy, length_y, depth)
        x_from, x_to, x_n = span(dx, length_x, depth)
        if x_to < 0:
            x_to += width
        k = used[0]
        used[0] += 1
        copy = pltpu.make_async_remote_copy(
            src_ref=src.at[pl.ds(off_src + y_from, y_n), pl.ds(x_from, x_n), :],
            dst_ref=dst.at[pl.ds(off_dst + y_to, y_n), pl.ds(x_to, x_n), :],
            send_sem=send.at[k],
            recv_sem=recv.at[k],
            device_id=device(dy, dx),
            device_id_type=MESH,
        )
        copy.start()
        return copy

    def fine_sends(src, dst, off_src, depth, around):
        out = []
        for dy, dx in around:
            deep = 1 if dy != 0 and dx != 0 else depth
            out.append(send_to(dy, dx, src, dst, deep, ny, nx, off_src, DEEP))
        return out

    def coarse_sends(ref):
        return [send_to(dy, dx, ref, ref, WIDE, cy, cx, WIDE, WIDE) for dy, dx in CORNERS + SIDES]

    def finish(copies):
        for copy in copies:
            copy.wait()

    def inside(ref):
        return ref.at[pl.ds(DEEP, ny), pl.ds(0, nx), :]

    loads = []
    for k, (src, dst) in enumerate(((m_hbm, m), (u_hbm, a), (f_hbm, f))):
        copy = pltpu.make_async_copy(src, inside(dst), local.at[k])
        copy.start()
        loads.append(copy)
    pl.semaphore_wait(barrier, len(AROUND))
    first = fine_sends(u_hbm, a, 0, DEEP, AROUND)
    first += fine_sends(m_hbm, m, 0, 1, SIDES)
    first += fine_sends(f_hbm, f, 0, 1, SIDES)

    halves = [pl.ds(h * LANES, LANES) for h in range(nl // LANES)]

    def cross(src, r, lane, width):
        mid = src[r, :, lane]
        left = pltpu.roll(mid, 1, 0)
        right = pltpu.roll(mid, wide_x - 1, 0)
        total = (left + right)[:width] + (src[r - 1, pl.ds(0, width), lane] + src[r + 1, pl.ds(0, width), lane])
        return mid[:width], total

    def sweep(src, dst, low, high, width):
        def body(r, carry):
            for lane in halves:
                mid, total = cross(src, r, lane, width)
                part = pl.ds(0, width)
                dst[r, part, lane] = 0.2 * mid + w[r, part, lane] * (total + f[r, part, lane])
            return carry

        lax.fori_loop(DEEP + low, DEEP + high, body, 0)

    def defect(src, r, lane):
        mid, total = cross(src, r, lane, nx)
        part = pl.ds(0, nx)
        return f[r, part, lane] + total - (4.0 + m[r, part, lane]) * mid

    at_block = lax.broadcasted_iota(jnp.int32, (cx, nx), 0)
    of_cell = lax.broadcasted_iota(jnp.int32, (cx, nx), 1) // RATIO
    pool = jnp.where(at_block == of_cell, 1.0 / RATIO, 0.0).astype(jnp.float32)
    of_row = lax.broadcasted_iota(jnp.int32, (nx, cx), 0) // RATIO
    at_row = lax.broadcasted_iota(jnp.int32, (nx, cx), 1)
    unpool = jnp.where(of_row == at_row, 1.0, 0.0).astype(jnp.float32)

    def dot(left, right):
        return jnp.dot(left, right, precision=lax.Precision.HIGHEST, preferred_element_type=jnp.float32)

    loads[0].wait()

    def masses(j, carry):
        for lane in halves:
            rows4 = [m[DEEP + j * RATIO + i, pl.ds(0, nx), lane] for i in range(RATIO)]
            cm[WIDE + j, pl.ds(0, cx), lane] = dot(pool, (rows4[0] + rows4[1]) + (rows4[2] + rows4[3]))
        return carry

    lax.fori_loop(0, cy, masses, 0)
    loads[1].wait()
    loads[2].wait()
    finish(first)
    mass_copies = coarse_sends(cm)

    def factor(r, carry):
        for lane in halves:
            w[r, :, lane] = 0.8 / (4.0 + m[r, :, lane])
        return carry

    lax.fori_loop(DEEP - 1, DEEP + ny + 1, factor, 0)

    sweep(a, b, -1, ny + 1, wide_x)
    sweep(b, c, 0, ny, nx)
    finish(fine_sends(c, c, DEEP, DEEP, AROUND))
    sweep(c, b, -1, ny + 1, wide_x)

    def coarse_loads(j, carry):
        for lane in halves:
            d = [defect(b, DEEP + j * RATIO + i, lane) for i in range(RATIO)]
            cl[WIDE + j, pl.ds(0, cx), lane] = dot(pool, (d[0] + d[1]) + (d[2] + d[3]))
        return carry

    lax.fori_loop(0, cy, coarse_loads, 0)
    load_copies = coarse_sends(cl)
    finish(mass_copies)

    def coarse_factor(r, carry):
        cw[r] = 0.8 / (4.0 + cm[r])
        return carry

    lax.fori_loop(0, cy + 2 * WIDE, coarse_factor, 0)
    finish(load_copies)

    def coarse_first(r, carry):
        v0[r] = cw[r] * cl[r]
        return carry

    lax.fori_loop(0, cy + 2 * WIDE, coarse_first, 0)

    def coarse_sweep(src, dst, edge, width):
        def body(r, carry):
            mid = src[r]
            total = pltpu.roll(mid, 1, 0) + pltpu.roll(mid, wide_cx - 1, 0) + (src[r - 1] + src[r + 1])
            new = 0.2 * mid + cw[r] * (total + cl[r])
            dst[r, pl.ds(0, width), :] = new[:width]
            return carry

        lax.fori_loop(edge, cy + 2 * WIDE - edge, body, 0, unroll=2)

    src = v0
    done, edge = 1, 0
    while done < INNER:
        edge += 1
        done += 1
        if edge == WIDE and done < INNER:
            coarse_sweep(src, v5, edge, cx)
            finish(coarse_sends(v5))
            src, edge = v5, 0
        else:
            dst = v1 if src is v0 else v0
            coarse_sweep(src, dst, edge, wide_cx)
            src = dst
    coarse = src

    def correct(j, carry):
        for lane in halves:
            add = dot(unpool, coarse[WIDE + j, pl.ds(0, cx), lane])
            for i in range(RATIO):
                r = DEEP + j * RATIO + i
                a[r, pl.ds(0, nx), lane] = b[r, pl.ds(0, nx), lane] + add
        return carry

    lax.fori_loop(0, cy, correct, 0)
    finish(fine_sends(a, a, DEEP, DEEP, AROUND))
    sweep(a, b, -1, ny + 1, wide_x)
    sweep(b, c, 0, ny, nx)
    finish(fine_sends(c, c, DEEP, DEEP, AROUND))
    sweep(c, b, -1, ny + 1, wide_x)
    outs = []
    copy = pltpu.make_async_copy(inside(b), out_hbm, local.at[3])
    copy.start()
    outs.append(copy)
    chunks = 4
    size = ny // chunks
    for k in range(chunks):
        def rest(r, carry):
            for lane in halves:
                a[r, pl.ds(0, nx), lane] = defect(b, r, lane)
            return carry

        lax.fori_loop(DEEP + k * size, DEEP + (k + 1) * size, rest, 0)
        copy = pltpu.make_async_copy(
            a.at[pl.ds(DEEP + k * size, size), pl.ds(0, nx), :], rem_hbm.at[pl.ds(k * size, size)], local.at[4 + k])
        copy.start()
        outs.append(copy)
    finish(outs)


def solution(mesh):
    rows, cols = mesh.shape["row"], mesh.shape["col"]

    def local(source_terms, initial_values, absorption):
        ny, nx, nl = source_terms.shape
        fine = pltpu.VMEM((ny + 2 * DEEP, nx + TILE, nl), jnp.float32)
        coarse = pltpu.VMEM((ny // RATIO + 2 * WIDE, nx // RATIO + TILE, nl), jnp.float32)
        anywhere = pl.BlockSpec(memory_space=pl.ANY)
        result = jax.ShapeDtypeStruct((ny, nx, nl), jnp.float32)
        return pl.pallas_call(
            functools.partial(kernel, rows, cols, ny, nx, nl),
            out_shape=(result, result),
            in_specs=[anywhere] * 3,
            out_specs=(anywhere, anywhere),
            scratch_shapes=[fine] * 6 + [coarse] * 6 + [
                pltpu.SemaphoreType.DMA((72,)),
                pltpu.SemaphoreType.DMA((72,)),
                pltpu.SemaphoreType.DMA((8,)),
            ],
            compiler_params=pltpu.CompilerParams(
                collective_id=0, has_side_effects=True, vmem_limit_bytes=48 * 1024 * 1024),
            name="two_grids",
        )(source_terms, initial_values, absorption)

    spec = P("row", "col", None)
    return jax.shard_map(local, mesh=mesh, in_specs=(spec,) * 3, out_specs=(spec,) * 2, check_vma=False)
```

```python
import functools

import jax
import jax.numpy as jnp
from jax import lax
from jax.experimental import pallas as pl
from jax.experimental.pallas import tpu as pltpu
from jax.sharding import PartitionSpec as P

RATIO = 4
INNER = 9
DEEP = 2
WIDE = 4
TILE = 8
UNROLL = 2
LANES = 128
MESH = pl.DeviceIdType.MESH
SIDES = ((-1, 0), (1, 0), (0, -1), (0, 1))
CORNERS = ((-1, -1), (-1, 1), (1, -1), (1, 1))
AROUND = SIDES + CORNERS


def span(step, length, depth):
    if step == 0:
        return 0, 0, length
    if step < 0:
        return 0, length, depth
    return length - depth, -depth, depth


def kernel(rows, cols, ny, nx, nl, f_hbm, u_hbm, m_hbm, out_hbm, rem_hbm, a, b, c, f, m, w, cl, cm, cw, v0, v1, v5,
           send, recv, local):
    me_r, me_c = lax.axis_index("row"), lax.axis_index("col")
    cy, cx = ny // RATIO, nx // RATIO
    wide_x, wide_cx = nx + TILE, cx + TILE

    def device(dy, dx):
        return (lax.rem(me_r + (dy + rows), rows), lax.rem(me_c + (dx + cols), cols))

    barrier = pltpu.get_barrier_semaphore()
    for dy, dx in AROUND:
        pl.semaphore_signal(barrier, inc=1, device_id=device(dy, dx), device_id_type=MESH)

    used = [0]

    def send_to(dy, dx, src, dst, depth, length_y, length_x, off_src, off_dst):
        width = length_x + TILE
        y_from, y_to, y_n = span(dy, length_y, depth)
        x_from, x_to, x_n = span(dx, length_x, depth)
        if x_to < 0:
            x_to += width
        k = used[0]
        used[0] += 1
        copy = pltpu.make_async_remote_copy(
            src_ref=src.at[pl.ds(off_src + y_from, y_n), pl.ds(x_from, x_n), :],
            dst_ref=dst.at[pl.ds(off_dst + y_to, y_n), pl.ds(x_to, x_n), :],
            send_sem=send.at[k],
            recv_sem=recv.at[k],
            device_id=device(dy, dx),
            device_id_type=MESH,
        )
        copy.start()
        return copy

    def fine_sends(src, dst, off_src, depth, around):
        out = []
        for dy, dx in around:
            deep = 1 if dy != 0 and dx != 0 else depth
            out.append(send_to(dy, dx, src, dst, deep, ny, nx, off_src, DEEP))
        return out

    def corner_row(dy, dx, ref, i):
        n = WIDE - 1 - i
        k = used[0]
        used[0] += 1
        copy = pltpu.make_async_remote_copy(
            src_ref=ref.at[pl.ds(WIDE + (i if dy < 0 else cy - 1 - i), 1), pl.ds(0 if dx < 0 else cx - n, n), :],
            dst_ref=ref.at[pl.ds(WIDE + cy + i if dy < 0 else WIDE - 1 - i, 1), pl.ds(cx if dx < 0 else wide_cx - n, n), :],
            send_sem=send.at[k],
            recv_sem=recv.at[k],
            device_id=device(dy, dx),
            device_id_type=MESH,
        )
        copy.start()
        return copy

    def coarse_sends(ref):
        out = [corner_row(dy, dx, ref, i) for i in range(WIDE - 1) for dy, dx in CORNERS]
        return out + [send_to(dy, dx, ref, ref, WIDE, cy, cx, WIDE, WIDE) for dy, dx in SIDES[2:] + SIDES[:2]]

    def finish(copies):
        for copy in copies:
            copy.wait()

    def inside(ref):
        return ref.at[pl.ds(DEEP, ny), pl.ds(0, nx), :]

    loads = []
    for k, (src, dst) in enumerate(((m_hbm, m), (u_hbm, a), (f_hbm, f))):
        copy = pltpu.make_async_copy(src, inside(dst), local.at[k])
        copy.start()
        loads.append(copy)
    pl.semaphore_wait(barrier, len(AROUND))
    first = fine_sends(u_hbm, a, 0, DEEP, AROUND)
    first += fine_sends(m_hbm, m, 0, 1, SIDES)
    first += fine_sends(f_hbm, f, 0, 1, SIDES)

    halves = [pl.ds(h * LANES, LANES) for h in range(nl // LANES)]

    def cross(src, r, lane, width):
        mid = src[r, :, lane]
        left = pltpu.roll(mid, 1, 0)
        right = pltpu.roll(mid, wide_x - 1, 0)
        total = (left + right)[:width] + (src[r - 1, pl.ds(0, width), lane] + src[r + 1, pl.ds(0, width), lane])
        return mid[:width], total

    def full_row(src, dst, r, width):
        for lane in halves:
            mid, total = cross(src, r, lane, width)
            part = pl.ds(0, width)
            dst[r, part, lane] = 0.2 * mid + w[r, part, lane] * (total + f[r, part, lane])

    def full_rows(src, dst, low, high, width):
        def body(r, carry):
            full_row(src, dst, DEEP + r, width)
            full_row(src, dst, DEEP + ny - 1 - r, width)
            return carry

        lax.fori_loop(low, high, body, 0)

    def middle(src, dst, low):
        part = pl.ds(TILE, nx - 2 * TILE)

        def body(r, carry):
            for lane in halves:
                line = src[r, pl.ds(0, nx), lane]
                beside = (pltpu.roll(line, 1, 0) + pltpu.roll(line, nx - 1, 0))[TILE:nx - TILE]
                total = beside + (src[r - 1, part, lane] + src[r + 1, part, lane])
                dst[r, part, lane] = 0.2 * line[TILE:nx - TILE] + w[r, part, lane] * (total + f[r, part, lane])
            return carry

        lax.fori_loop(DEEP + low, DEEP + ny - low, body, 0, unroll=UNROLL)

    def edges(src, dst, low, halo):
        last = pl.ds(nx - TILE, 2 * TILE)
        begin = pl.ds(0, TILE)

        def body(r, carry):
            for lane in halves:
                line = jnp.concatenate([src[r, pl.ds(nx - 2 * TILE, 3 * TILE), lane], src[r, pl.ds(0, 2 * TILE), lane]], axis=0)
                size = 5 * TILE
                beside = (pltpu.roll(line, 1, 0) + pltpu.roll(line, size - 1, 0))
                at_end = beside[TILE:3 * TILE] + (src[r - 1, last, lane] + src[r + 1, last, lane])
                at_end = 0.2 * line[TILE:3 * TILE] + w[r, last, lane] * (at_end + f[r, last, lane])
                if halo:
                    dst[r, last, lane] = at_end
                else:
                    dst[r, pl.ds(nx - TILE, TILE), lane] = at_end[:TILE]
                at_begin = beside[3 * TILE:4 * TILE] + (src[r - 1, begin, lane] + src[r + 1, begin, lane])
                dst[r, begin, lane] = 0.2 * line[3 * TILE:4 * TILE] + w[r, begin, lane] * (at_begin + f[r, begin, lane])
            return carry

        lax.fori_loop(DEEP + low, DEEP + ny - low, body, 0, unroll=UNROLL)

    def first_sweep(src, dst, between):
        middle(src, dst, 1)
        between()
        full_rows(src, dst, -1, 1, wide_x)
        edges(src, dst, 1, True)

    def second_sweep(src, dst):
        full_rows(src, dst, 0, DEEP, nx)
        edges(src, dst, DEEP, False)
        copies = fine_sends(dst, dst, DEEP, DEEP, SIDES[2:] + CORNERS + SIDES[:2])
        middle(src, dst, DEEP)
        return copies

    def defect(src, r, lane):
        mid, total = cross(src, r, lane, nx)
        part = pl.ds(0, nx)
        return f[r, part, lane] + total - (4.0 + m[r, part, lane]) * mid

    at_block = lax.broadcasted_iota(jnp.int32, (cx, nx), 0)
    of_cell = lax.broadcasted_iota(jnp.int32, (cx, nx), 1) // RATIO
    pool = jnp.where(at_block == of_cell, 1.0 / RATIO, 0.0).astype(jnp.float32)
    of_row = lax.broadcasted_iota(jnp.int32, (nx, cx), 0) // RATIO
    at_row = lax.broadcasted_iota(jnp.int32, (nx, cx), 1)
    unpool = jnp.where(of_row == at_row, 1.0, 0.0).astype(jnp.float32)

    def dot(left, right):
        return jnp.dot(left, right, precision=lax.Precision.HIGHEST, preferred_element_type=jnp.float32)

    loads[0].wait()

    def masses(j, carry):
        for lane in halves:
            rows4 = [m[DEEP + j * RATIO + i, pl.ds(0, nx), lane] for i in range(RATIO)]
            cm[WIDE + j, pl.ds(0, cx), lane] = dot(pool, (rows4[0] + rows4[1]) + (rows4[2] + rows4[3]))
        return carry

    lax.fori_loop(0, cy, masses, 0)
    def factor(low, high, part):
        def body(r, carry):
            w[r, part, :] = 0.8 / (4.0 + m[r, part, :])
            return carry

        lax.fori_loop(low, high, body, 0)

    factor(DEEP, DEEP + ny, pl.ds(0, nx))
    loads[1].wait()
    loads[2].wait()
    mass_copies = []

    def arrived():
        finish(first)
        mass_copies.extend(coarse_sends(cm))
        factor(DEEP, DEEP + ny, pl.ds(nx, TILE))
        factor(DEEP - 1, DEEP, pl.ds(0, wide_x))
        factor(DEEP + ny, DEEP + ny + 1, pl.ds(0, wide_x))

    first_sweep(a, b, arrived)
    copies = second_sweep(b, c)
    first_sweep(c, b, lambda: finish(copies))

    def coarse_loads(j, carry):
        for lane in halves:
            d = [defect(b, DEEP + j * RATIO + i, lane) for i in range(RATIO)]
            cl[WIDE + j, pl.ds(0, cx), lane] = dot(pool, (d[0] + d[1]) + (d[2] + d[3]))
        return carry

    lax.fori_loop(0, cy, coarse_loads, 0)
    load_copies = coarse_sends(cl)
    finish(mass_copies)

    def coarse_factor(r, carry):
        cw[r] = 0.8 / (4.0 + cm[r])
        return carry

    lax.fori_loop(0, cy + 2 * WIDE, coarse_factor, 0)
    finish(load_copies)

    def coarse_first(r, carry):
        v0[r] = cw[r] * cl[r]
        return carry

    lax.fori_loop(0, cy + 2 * WIDE, coarse_first, 0)

    def coarse_sweep(src, dst, edge, width):
        def body(r, carry):
            mid = src[r]
            total = pltpu.roll(mid, 1, 0) + pltpu.roll(mid, wide_cx - 1, 0) + (src[r - 1] + src[r + 1])
            new = 0.2 * mid + cw[r] * (total + cl[r])
            dst[r, pl.ds(0, width), :] = new[:width]
            return carry

        lax.fori_loop(edge, cy + 2 * WIDE - edge, body, 0, unroll=2)

    src = v0
    done, edge = 1, 0
    while done < INNER:
        edge += 1
        done += 1
        if edge == WIDE and done < INNER:
            coarse_sweep(src, v5, edge, cx)
            finish(coarse_sends(v5))
            src, edge = v5, 0
        else:
            dst = v1 if src is v0 else v0
            coarse_sweep(src, dst, edge, wide_cx)
            src = dst
    coarse = src

    def correct(j, carry):
        for lane in halves:
            add = dot(unpool, coarse[WIDE + j, pl.ds(0, cx), lane])
            for i in range(RATIO):
                r = DEEP + j * RATIO + i
                a[r, pl.ds(0, nx), lane] = b[r, pl.ds(0, nx), lane] + add
        return carry

    lax.fori_loop(0, cy, correct, 0)
    copies = fine_sends(a, a, DEEP, DEEP, SIDES[2:] + CORNERS + SIDES[:2])
    first_sweep(a, b, lambda: finish(copies))
    copies = second_sweep(b, c)
    first_sweep(c, b, lambda: finish(copies))
    outs = []
    copy = pltpu.make_async_copy(inside(b), out_hbm, local.at[3])
    copy.start()
    outs.append(copy)
    chunks = 4
    size = ny // chunks
    for k in range(chunks):
        def rest(r, carry):
            for lane in halves:
                a[r, pl.ds(0, nx), lane] = defect(b, r, lane)
            return carry

        lax.fori_loop(DEEP + k * size, DEEP + (k + 1) * size, rest, 0)
        copy = pltpu.make_async_copy(
            a.at[pl.ds(DEEP + k * size, size), pl.ds(0, nx), :], rem_hbm.at[pl.ds(k * size, size)], local.at[4 + k])
        copy.start()
        outs.append(copy)
    finish(outs)


def solution(mesh):
    rows, cols = mesh.shape["row"], mesh.shape["col"]

    def local(source_terms, initial_values, absorption):
        ny, nx, nl = source_terms.shape
        fine = pltpu.VMEM((ny + 2 * DEEP, nx + TILE, nl), jnp.float32)
        coarse = pltpu.VMEM((ny // RATIO + 2 * WIDE, nx // RATIO + TILE, nl), jnp.float32)
        anywhere = pl.BlockSpec(memory_space=pl.ANY)
        result = jax.ShapeDtypeStruct((ny, nx, nl), jnp.float32)
        return pl.pallas_call(
            functools.partial(kernel, rows, cols, ny, nx, nl),
            out_shape=(result, result),
            in_specs=[anywhere] * 3,
            out_specs=(anywhere, anywhere),
            scratch_shapes=[fine] * 6 + [coarse] * 6 + [
                pltpu.SemaphoreType.DMA((112,)),
                pltpu.SemaphoreType.DMA((112,)),
                pltpu.SemaphoreType.DMA((8,)),
            ],
            compiler_params=pltpu.CompilerParams(
                collective_id=0, has_side_effects=True, vmem_limit_bytes=48 * 1024 * 1024),
            name="two_grids",
        )(source_terms, initial_values, absorption)

    spec = P("row", "col", None)
    return jax.shard_map(local, mesh=mesh, in_specs=(spec,) * 3, out_specs=(spec,) * 2, check_vma=False)
```
